32 devices in a mesh: row: 2 (over y), col: 8 (over z, x), rep: 2 (over core).
Axes of the slice: x: 2, y: 2, z: 4, core: 2. Of those that a mesh axis runs over, the one named last changes fastest.
Arguments:
- gain: float32 [48, 8, 128, 128], P(('row', 'col'), 'rep'), as said below
- coupled_columns: int32 [48, 8], P(('row', 'col')), may hold values from 0 to 47, as said below
- solution: float32 [6144, 512], P(('row', 'col')), may hold values from -6 to 6
- residual: float32 [6144, 512], P(('row', 'col')), may hold values from -6 to 6
- direction: float32 [6144, 512], P(('row', 'col')), may hold values from -6 to 6
Outputs:
- solution_next: float32 [6144, 512], P(('row', 'col'))
- residual_next: float32 [6144, 512], P(('row', 'col'))
- direction_next: float32 [6144, 512], P(('row', 'col'))
The draws below stay inside these ranges and needn't reach their ends.
Inputs may be any that keep to these rules, and one draw needn't show every extreme that they name: `coupled_columns`: each block row i names first its coupled block columns in ascending order (always i - 1, i, i + 1 where inside 0 to 47, some of i - 3, i - 2, i + 2, i + 3, the coupling being symmetric), at most 7 of them, and then fills the remaining slots with i itself; every named column is within 3 of i. The gain matrix assembled from its blocks is symmetric; padding slots hold zero blocks; each diagonal entry exceeds the sum of the absolute values of the other entries of its row by exactly 1.
All inputs are finite; a program needn't handle non-finite values.
Results may differ from the reference program's by a relative error of at most 0.000061.
Values sent between devices are 32-bit elements; how exact they have to be, the bound alone decides.
A program may use at most 64 MiB of HBM per device.

```python
import jax
import jax.numpy as jnp
from jax import lax

BLK = 128
SNAP = 512
NB = 48
NS = 6144


reach_blocks = 3


def coupling_layout(key):
    coupling_bits = jax.random.randint(jax.random.fold_in(key, 11), (2, NB), 0, 2).astype(jnp.int32)
    positions = jnp.arange(NB, dtype=jnp.int32)
    offsets = jnp.arange(-reach_blocks, reach_blocks + 1, dtype=jnp.int32)
    targets = positions[:, None] + offsets[None, :]
    inside = jnp.logical_and(targets >= 0, targets < NB)
    always = jnp.ones((NB,), jnp.int32)
    chosen = jnp.stack([jnp.roll(coupling_bits[1], 3), jnp.roll(coupling_bits[0], 2), always, always, always, coupling_bits[0], coupling_bits[1]], axis=1)
    present = jnp.logical_and(inside, chosen == 1)
    slot_keys = jnp.where(present, 0, 16) + offsets[None, :] + reach_blocks
    ordering = jnp.argsort(slot_keys, axis=1, stable=True).astype(jnp.int32)
    present_sorted = jnp.take_along_axis(present, ordering, axis=1)
    targets_sorted = jnp.take_along_axis(targets, ordering, axis=1)
    columns = jnp.where(present_sorted, targets_sorted, positions[:, None])
    columns = jnp.concatenate([columns, positions[:, None]], axis=1).astype(jnp.int32)
    return (present, ordering, columns)


def draw_coupled_columns(key, part):
    present, ordering, columns = coupling_layout(key)
    return columns


def draw_gain(key, part):
    present, ordering, columns = coupling_layout(key)
    spread_scale = (7.0 * BLK) ** (-0.5)
    pair_key = jax.random.fold_in(key, 23)
    own_key = jax.random.fold_in(key, 29)
    pair_noise = jax.random.normal(pair_key, (3, NB, BLK, BLK), jnp.float32) * spread_scale
    own_noise = jax.random.normal(own_key, (NB, BLK, BLK), jnp.float32) * spread_scale
    identity = jnp.eye(BLK, dtype=jnp.float32)
    own_noise = (own_noise + jnp.transpose(own_noise, (0, 2, 1))) * 0.5 * (1.0 - identity)[None]
    upper_blocks = [pair_noise[0], pair_noise[1], pair_noise[2]]
    lower_blocks = [jnp.transpose(jnp.roll(pair_noise[step], step + 1, axis=0), (0, 2, 1)) for step in range(3)]
    stacked = jnp.stack([lower_blocks[2], lower_blocks[1], lower_blocks[0], own_noise, upper_blocks[0], upper_blocks[1], upper_blocks[2]], axis=1)
    stacked = stacked * present[:, :, None, None].astype(jnp.float32)
    dominant = 1.0 + jnp.sum(jnp.abs(stacked), axis=(1, 3))
    diagonal_block = stacked[:, 3] + identity[None] * dominant[:, :, None]
    stacked = stacked.at[:, 3].set(diagonal_block)
    sorted_blocks = jnp.take_along_axis(stacked, ordering[:, :, None, None], axis=1)
    padding = jnp.zeros((NB, 1, BLK, BLK), jnp.float32)
    return jnp.concatenate([sorted_blocks, padding], axis=1)


def shard_levels(key, shape, shards, low, top_value):
    level, own = 1.0, jax.random.fold_in(key, 6)
    for axis_at, shards_of in shards:
        steps = jnp.exp(jax.random.uniform(jax.random.fold_in(own, axis_at), (shards_of,), jnp.float32, low / len(shards), top_value / len(shards)))
        level = level * jnp.repeat(steps, shape[axis_at] // shards_of).reshape([-1 if axis == axis_at else 1 for axis in range(len(shape))])
    return level


def gaussian(key, dims, deviation, reach, shards=(), kind=jnp.bfloat16):
    array = deviation * jax.random.normal(key, dims, jnp.float32)
    if shards:
        array = array * shard_levels(key, dims, shards, -0.22, 0.18)
    return jnp.clip(array, -reach, reach).astype(kind)


def setup_inputs(seed: int = 0) -> dict:
    key_list = jax.random.split(jax.random.key(seed), 6)
    return {
        "gain": draw_gain(jax.random.fold_in(key_list[5], 71), 0),
        "coupled_columns": draw_coupled_columns(jax.random.fold_in(key_list[5], 71), 0),
        "solution": gaussian(key_list[2], (NS, SNAP), 1.0, 6.0, ((0, 16),), jnp.float32),
        "residual": gaussian(key_list[3], (NS, SNAP), 1.0, 6.0, ((0, 16),), jnp.float32),
        "direction": gaussian(key_list[4], (NS, SNAP), 1.0, 6.0, ((0, 16),), jnp.float32),
    }


def reference(gain, coupled_columns, solution, residual, direction):
    snapshots = direction.shape[1]
    segments = direction.reshape(NB, BLK, snapshots)

    def one_row(block_row):
        blocks = gain[block_row]
        picked = segments[coupled_columns[block_row]]
        return jnp.einsum("kab,kbs->as", blocks, picked, precision=lax.Precision.HIGHEST, preferred_element_type=jnp.float32)

    image = lax.map(one_row, jnp.arange(NB, dtype=jnp.int32)).reshape(NS, snapshots)
    norm_old = jnp.sum(residual * residual, axis=0)
    curvature = jnp.sum(direction * image, axis=0)
    step_size = norm_old / curvature
    solution_next = solution + step_size * direction
    residual_next = residual - step_size * image
    norm_new = jnp.sum(residual_next * residual_next, axis=0)
    direction_next = residual_next + (norm_new / norm_old) * direction
    return solution_next, residual_next, direction_next
```

```python
import functools

import jax
import jax.numpy as jnp
from jax import lax
from jax.experimental import pallas as pl
from jax.experimental.pallas import tpu as pltpu
from jax.sharding import PartitionSpec as P

BLK = 128
LANES = 128
DIRECT_LIMIT = 16
CHUNK_ROWS = 64
MESH = pl.DeviceIdType.MESH


def split_bf16(value):
    high = value.astype(jnp.bfloat16)
    low = (value - high.astype(jnp.float32)).astype(jnp.bfloat16)
    return high, low


def iteration_kernel(
    sizes,
    columns_ref, gain_hbm, solution_hbm, residual_hbm, direction_hbm,
    solution_out, residual_out, direction_out,
    own_dir, own_res, own_sol, gains, near, far, band_high, band_low, images, totals, *rest,
):
    rows_n, cols_n = sizes
    segments = rows_n * cols_n
    direct = segments <= DIRECT_LIMIT
    phase_count = 1 if direct else 2
    parts = rest[:phase_count]
    part_send = rest[phase_count:2 * phase_count]
    part_recv = rest[2 * phase_count:3 * phase_count]
    (near_send, near_recv, far_send, far_recv, pair_send, pair_recv, local_sem) = rest[3 * phase_count:]

    seg_rows, half = near.shape
    block_rows = seg_rows // BLK
    slots_half = gains.shape[2]
    tiles = half // LANES
    chunks = seg_rows // CHUNK_ROWS

    row, col, rep = lax.axis_index("row"), lax.axis_index("col"), lax.axis_index("rep")
    seg = row * cols_n + col
    odd = lax.rem(seg, 2)
    other = 1 - rep

    def at_segment(index):
        return {"row": index // cols_n, "col": lax.rem(index, cols_n), "rep": rep}

    partner = {"row": row, "col": col, "rep": other}
    near_id = at_segment(seg + 1 - 2 * odd)
    target = seg + 2 - 4 * odd
    source = seg - 2 + 4 * odd
    sends_far = jnp.logical_and(target >= 0, target < segments)
    gets_far = jnp.logical_and(source >= 0, source < segments)
    far_id = at_segment(jnp.clip(target, 0, segments - 1))
    source_id = at_segment(jnp.clip(source, 0, segments - 1))

    if direct:
        phases = [(seg, segments, at_segment)]
    else:
        phases = [
            (col, cols_n, lambda index: {"row": row, "col": index, "rep": rep}),
            (row, rows_n, lambda index: {"row": index, "col": col, "rep": rep}),
        ]

    barrier = pltpu.get_barrier_semaphore()

    def greet(device):
        pl.semaphore_signal(barrier, inc=1, device_id=device, device_id_type=MESH)

    own_cols = pl.ds(pl.multiple_of(rep * half, LANES), half)
    other_cols = pl.ds(pl.multiple_of(other * half, LANES), half)
    load_dir = pltpu.make_async_copy(direction_hbm.at[:, own_cols], own_dir.at[:, own_cols], local_sem.at[0])
    load_gain = pltpu.make_async_copy(gain_hbm, gains.at[rep], local_sem.at[1])
    load_res = pltpu.make_async_copy(residual_hbm, own_res, local_sem.at[2])
    load_dir_other = pltpu.make_async_copy(direction_hbm.at[:, other_cols], own_dir.at[:, other_cols], local_sem.at[3])
    load_sol = pltpu.make_async_copy(solution_hbm, own_sol, local_sem.at[4])

    greet(partner)
    waits = 1
    if not direct:
        greet(near_id)
        waits += 1
    for place, count, device_of in phases:
        for step in range(1, count):
            greet(device_of(lax.rem(place + step, count)))
        waits += count - 1
    if not direct:
        @pl.when(sends_far)
        def _():
            greet(far_id)

        @pl.when(gets_far)
        def _():
            greet(source_id)

    load_dir.start()
    load_gain.start()
    load_res.start()
    load_dir_other.start()
    load_sol.start()

    pl.semaphore_wait(barrier, waits)
    if not direct:
        @pl.when(sends_far)
        def _():
            pl.semaphore_wait(barrier, 1)

        @pl.when(gets_far)
        def _():
            pl.semaphore_wait(barrier, 1)

    def near_copy(chunk):
        part = pl.ds(chunk * CHUNK_ROWS, CHUNK_ROWS)
        return pltpu.make_async_remote_copy(
            src_ref=own_dir.at[part, own_cols], dst_ref=near.at[part],
            send_sem=near_send.at[chunk], recv_sem=near_recv.at[chunk],
            device_id=near_id, device_id_type=MESH,
        )

    def far_copy(chunk):
        part = pl.ds(chunk * CHUNK_ROWS, CHUNK_ROWS)
        return pltpu.make_async_remote_copy(
            src_ref=near.at[part], dst_ref=far.at[part],
            send_sem=far_send.at[chunk], recv_sem=far_recv.at[chunk],
            device_id=far_id, device_id_type=MESH,
        )

    def pair_copy(index, src, dst):
        return pltpu.make_async_remote_copy(
            src_ref=src, dst_ref=dst, send_sem=pair_send.at[index], recv_sem=pair_recv.at[index],
            device_id=partner, device_id_type=MESH,
        )

    load_dir.wait()
    for chunk in range(chunks):
        near_copy(chunk).start()
    gain_pair = pair_copy(0, gain_hbm, gains.at[rep])
    gain_pair.start()

    first_block = seg * block_rows
    bases = (first_block, first_block + block_rows * (1 - 2 * odd), first_block - block_rows * (1 - 2 * odd))

    def build_band(group):
        for r in range(block_rows):
            names = [columns_ref[r, k] for k in range(2 * slots_half)]
            for j in range(block_rows):
                wanted = bases[group] + j
                slot = jnp.int32(0)
                found = jnp.float32(0)
                for k in reversed(range(2 * slots_half)):
                    match = names[k] == wanted
                    slot = jnp.where(match, k, slot)
                    found = jnp.where(match, jnp.float32(1), found)
                block = gains[slot // slots_half, r, lax.rem(slot, slots_half)] * found
                high, low = split_bf16(block)
                at = (group, pl.ds(r * BLK, BLK), pl.ds(j * BLK, BLK))
                band_high[at] = high
                band_low[at] = low

    def product(group, value):
        high, low = split_bf16(value)
        dot = functools.partial(jnp.dot, preferred_element_type=jnp.float32)
        return dot(band_high[group], high) + (dot(band_high[group], low) + dot(band_low[group], high))

    def tile_cols(side, tile):
        return pl.ds(pl.multiple_of(side * half + tile * LANES, LANES), LANES)

    def start_parts():
        load_res.wait()
        for tile in range(tiles):
            value = own_res[:, tile_cols(rep, tile)]
            parts[0][phases[0][0], pl.ds(tile, 1), :] = jnp.sum(value * value, axis=0, keepdims=True)

    def own_product():
        images[rep] = product(0, own_dir[:, own_cols])

    def gain_ready():
        load_gain.wait()
        gain_pair.wait()
        build_band(0)

    pieces = {0: start_parts, 1: gain_ready, 2: own_product, 3: lambda: build_band(1), 4: lambda: build_band(2)}
    for chunk in range(chunks):
        near_copy(chunk).wait_recv()

        @pl.when(sends_far)
        def _():
            far_copy(chunk).start()

        if chunk in pieces:
            pieces[chunk]()
    images[rep] += product(1, near[...])

    @pl.when(gets_far)
    def _():
        for chunk in range(chunks):
            far_copy(chunk).wait_recv()

    @pl.when(jnp.logical_not(gets_far))
    def _():
        far[...] = jnp.zeros_like(far)

    images[rep] += product(2, far[...])

    place0 = phases[0][0]
    for tile in range(tiles):
        image = images[rep, :, pl.ds(tile * LANES, LANES)]
        cols = tile_cols(rep, tile)
        for at, value in enumerate((own_dir[:, cols] * image, own_res[:, cols] * image, image * image)):
            parts[0][place0, pl.ds((at + 1) * tiles + tile, 1), :] = jnp.sum(value, axis=0, keepdims=True)

    image_pair = pair_copy(1, images.at[rep], images.at[rep])
    image_pair.start()

    for phase, (place, count, device_of) in enumerate(phases):
        copies = []
        for step in range(1, count):
            copies.append(pltpu.make_async_remote_copy(
                src_ref=parts[phase].at[place], dst_ref=parts[phase].at[place],
                send_sem=part_send[phase].at[step], recv_sem=part_recv[phase].at[step],
                device_id=device_of(lax.rem(place + step, count)), device_id_type=MESH,
            ))
        for copy in copies:
            copy.start()
        for copy in copies:
            copy.wait()
        total = parts[phase][0]
        for index in range(1, count):
            total = total + parts[phase][index]
        if phase + 1 < phase_count:
            parts[phase + 1][phases[phase + 1][0]] = total
        else:
            totals[rep] = total

    total_pair = pair_copy(2, totals.at[rep], totals.at[rep])
    total_pair.start()

    load_dir_other.wait()
    load_sol.wait()

    def update(side):
        for tile in range(tiles):
            norm_old, curvature, crossing, image_square = (
                totals[side, pl.ds(at * tiles + tile, 1), :] for at in range(4)
            )
            step_size = norm_old / curvature
            norm_new = norm_old - 2.0 * step_size * crossing + step_size * step_size * image_square
            scale = norm_new / norm_old
            cols = tile_cols(side, tile)
            direction = own_dir[:, cols]
            solution_out[:, cols] = own_sol[:, cols] + step_size * direction
            residual = own_res[:, cols] - step_size * images[side, :, pl.ds(tile * LANES, LANES)]
            residual_out[:, cols] = residual
            direction_out[:, cols] = residual + scale * direction

    update(rep)
    image_pair.wait()
    total_pair.wait()
    update(other)

    for chunk in range(chunks):
        near_copy(chunk).wait_send()

        @pl.when(sends_far)
        def _():
            far_copy(chunk).wait_send()


def solution(mesh):
    sizes = (mesh.shape["row"], mesh.shape["col"])
    segments = sizes[0] * sizes[1]
    counts = (segments,) if segments <= DIRECT_LIMIT else (sizes[1], sizes[0])

    def per_device(gain, coupled_columns, solution, residual, direction):
        seg_rows, snapshots = direction.shape
        half = snapshots // 2
        block_rows, slots_half = gain.shape[:2]
        chunks = seg_rows // CHUNK_ROWS
        sum_rows = 4 * (half // LANES)
        dma = pltpu.SemaphoreType.DMA
        whole = jax.ShapeDtypeStruct((seg_rows, snapshots), jnp.float32)
        any_space = pl.BlockSpec(memory_space=pl.ANY)
        vmem = pl.BlockSpec(memory_space=pltpu.VMEM)
        return pl.pallas_call(
            functools.partial(iteration_kernel, sizes),
            out_shape=(whole, whole, whole),
            in_specs=[pl.BlockSpec(memory_space=pltpu.SMEM), any_space, any_space, any_space, any_space],
            out_specs=(vmem, vmem, vmem),
            scratch_shapes=[
                pltpu.VMEM((seg_rows, snapshots), jnp.float32),
                pltpu.VMEM((seg_rows, snapshots), jnp.float32),
                pltpu.VMEM((seg_rows, snapshots), jnp.float32),
                pltpu.VMEM((2, block_rows, slots_half, BLK, BLK), jnp.float32),
                pltpu.VMEM((seg_rows, half), jnp.float32),
                pltpu.VMEM((seg_rows, half), jnp.float32),
                pltpu.VMEM((3, seg_rows, seg_rows), jnp.bfloat16),
                pltpu.VMEM((3, seg_rows, seg_rows), jnp.bfloat16),
                pltpu.VMEM((2, seg_rows, half), jnp.float32),
                pltpu.VMEM((2, sum_rows, LANES), jnp.float32),
                *[pltpu.VMEM((count, sum_rows, LANES), jnp.float32) for count in counts],
                *[dma((count,)) for count in counts],
                *[dma((count,)) for count in counts],
                dma((chunks,)), dma((chunks,)), dma((chunks,)), dma((chunks,)),
                dma((3,)), dma((3,)), dma((5,)),
            ],
            compiler_params=pltpu.CompilerParams(collective_id=0, has_side_effects=True),
            name="cg_iteration",
        )(coupled_columns, gain, solution, residual, direction)

    return jax.shard_map(
        per_device,
        mesh=mesh,
        in_specs=(
            P(("row", "col"), "rep", None, None),
            P(("row", "col"), None),
            P(("row", "col"), None),
            P(("row", "col"), None),
            P(("row", "col"), None),
        ),
        out_specs=(P(("row", "col"), None), P(("row", "col"), None), P(("row", "col"), None)),
        check_vma=False,
    )
```

```python
import functools

import jax
import jax.numpy as jnp
from jax import lax
from jax.experimental import pallas as pl
from jax.experimental.pallas import tpu as pltpu
from jax.sharding import PartitionSpec as P

BLK = 128
LANES = 128
DIRECT_LIMIT = 16
CHUNK_ROWS = 32
MESH = pl.DeviceIdType.MESH


def split_bf16(value):
    high = value.astype(jnp.bfloat16)
    low = (value - high.astype(jnp.float32)).astype(jnp.bfloat16)
    return high, low


def iteration_kernel(
    sizes,
    columns_ref, gain_hbm, solution_hbm, residual_hbm, direction_hbm,
    own_dir, own_res, own_sol, images, steps, scales,
    gains, near, far, band_high, band_low, totals, *rest,
):
    rows_n, cols_n = sizes
    segments = rows_n * cols_n
    direct = segments <= DIRECT_LIMIT
    phase_count = 1 if direct else 2
    parts = rest[:phase_count]
    part_send = rest[phase_count:2 * phase_count]
    part_recv = rest[2 * phase_count:3 * phase_count]
    (near_send, near_recv, far_send, far_recv, pair_send, pair_recv, local_sem) = rest[3 * phase_count:]

    seg_rows, half = near.shape
    block_rows = seg_rows // BLK
    slots_half = gains.shape[2]
    tiles = half // LANES
    chunks = seg_rows // CHUNK_ROWS

    row, col, rep = lax.axis_index("row"), lax.axis_index("col"), lax.axis_index("rep")
    seg = row * cols_n + col
    odd = lax.rem(seg, 2)
    other = 1 - rep

    def at_segment(index):
        return {"row": index // cols_n, "col": lax.rem(index, cols_n), "rep": rep}

    partner = {"row": row, "col": col, "rep": other}
    near_id = at_segment(seg + 1 - 2 * odd)
    target = seg + 2 - 4 * odd
    source = seg - 2 + 4 * odd
    sends_far = jnp.logical_and(target >= 0, target < segments)
    gets_far = jnp.logical_and(source >= 0, source < segments)
    far_id = at_segment(jnp.clip(target, 0, segments - 1))
    source_id = at_segment(jnp.clip(source, 0, segments - 1))

    if direct:
        phases = [(seg, segments, at_segment)]
    else:
        phases = [
            (col, cols_n, lambda index: {"row": row, "col": index, "rep": rep}),
            (row, rows_n, lambda index: {"row": index, "col": col, "rep": rep}),
        ]

    barrier = pltpu.get_barrier_semaphore()

    def greet(device):
        pl.semaphore_signal(barrier, inc=1, device_id=device, device_id_type=MESH)

    own_cols = pl.ds(pl.multiple_of(rep * half, LANES), half)
    other_cols = pl.ds(pl.multiple_of(other * half, LANES), half)
    load_dir = pltpu.make_async_copy(direction_hbm.at[:, own_cols], own_dir.at[:, own_cols], local_sem.at[0])
    load_gain = pltpu.make_async_copy(gain_hbm, gains.at[rep], local_sem.at[1])
    load_res = pltpu.make_async_copy(residual_hbm, own_res, local_sem.at[2])
    load_dir_other = pltpu.make_async_copy(direction_hbm.at[:, other_cols], own_dir.at[:, other_cols], local_sem.at[3])
    load_sol = pltpu.make_async_copy(solution_hbm, own_sol, local_sem.at[4])

    greet(partner)
    waits = 1
    if not direct:
        greet(near_id)
        waits += 1
    for place, count, device_of in phases:
        for step in range(1, count):
            greet(device_of(lax.rem(place + step, count)))
        waits += count - 1
    if not direct:
        @pl.when(sends_far)
        def _():
            greet(far_id)

        @pl.when(gets_far)
        def _():
            greet(source_id)

    load_dir.start()
    load_gain.start()
    load_res.start()
    load_dir_other.start()
    load_sol.start()

    pl.semaphore_wait(barrier, waits)
    if not direct:
        @pl.when(sends_far)
        def _():
            pl.semaphore_wait(barrier, 1)

        @pl.when(gets_far)
        def _():
            pl.semaphore_wait(barrier, 1)

    def near_copy(chunk):
        part = pl.ds(chunk * CHUNK_ROWS, CHUNK_ROWS)
        return pltpu.make_async_remote_copy(
            src_ref=own_dir.at[part, own_cols], dst_ref=near.at[part],
            send_sem=near_send.at[chunk], recv_sem=near_recv.at[chunk],
            device_id=near_id, device_id_type=MESH,
        )

    def far_copy(chunk):
        part = pl.ds(chunk * CHUNK_ROWS, CHUNK_ROWS)
        return pltpu.make_async_remote_copy(
            src_ref=near.at[part], dst_ref=far.at[part],
            send_sem=far_send.at[chunk], recv_sem=far_recv.at[chunk],
            device_id=far_id, device_id_type=MESH,
        )

    def pair_copy(index, src, dst):
        return pltpu.make_async_remote_copy(
            src_ref=src, dst_ref=dst, send_sem=pair_send.at[index], recv_sem=pair_recv.at[index],
            device_id=partner, device_id_type=MESH,
        )

    load_dir.wait()
    for chunk in range(chunks):
        near_copy(chunk).start()
    gain_pair = pair_copy(0, gain_hbm, gains.at[rep])
    gain_pair.start()

    first_block = seg * block_rows
    bases = (first_block, first_block + block_rows * (1 - 2 * odd), first_block - block_rows * (1 - 2 * odd))

    def build_band(group):
        for r in range(block_rows):
            names = [columns_ref[r, k] for k in range(2 * slots_half)]
            for j in range(block_rows):
                wanted = bases[group] + j
                slot = jnp.int32(0)
                found = jnp.float32(0)
                for k in reversed(range(2 * slots_half)):
                    match = names[k] == wanted
                    slot = jnp.where(match, k, slot)
                    found = jnp.where(match, jnp.float32(1), found)
                block = gains[slot // slots_half, r, lax.rem(slot, slots_half)] * found
                high, low = split_bf16(block)
                at = (group, pl.ds(r * BLK, BLK), pl.ds(j * BLK, BLK))
                band_high[at] = high
                band_low[at] = low

    def product(group, value):
        high, low = split_bf16(value)
        dot = functools.partial(jnp.dot, preferred_element_type=jnp.float32)
        return dot(band_high[group], high) + (dot(band_high[group], low) + dot(band_low[group], high))

    def tile_cols(side, tile):
        return pl.ds(pl.multiple_of(side * half + tile * LANES, LANES), LANES)

    def start_parts():
        load_res.wait()
        for tile in range(tiles):
            value = own_res[:, tile_cols(rep, tile)]
            parts[0][phases[0][0], pl.ds(tile, 1), :] = jnp.sum(value * value, axis=0, keepdims=True)

    def own_product():
        images[:, own_cols] = product(0, own_dir[:, own_cols])

    def gain_ready():
        load_gain.wait()
        gain_pair.wait()
        build_band(0)

    pieces = {0: start_parts, 1: gain_ready, 2: own_product, 3: lambda: build_band(1), 4: lambda: build_band(2)}
    for chunk in range(chunks):
        near_copy(chunk).wait_recv()

        @pl.when(sends_far)
        def _():
            far_copy(chunk).start()

        if chunk in pieces:
            pieces[chunk]()
    images[:, own_cols] += product(1, near[...])

    @pl.when(gets_far)
    def _():
        for chunk in range(chunks):
            far_copy(chunk).wait_recv()

    @pl.when(jnp.logical_not(gets_far))
    def _():
        far[...] = jnp.zeros_like(far)

    images[:, own_cols] += product(2, far[...])

    place0 = phases[0][0]
    for tile in range(tiles):
        cols = tile_cols(rep, tile)
        image = images[:, cols]
        for at, value in enumerate((own_dir[:, cols] * image, own_res[:, cols] * image, image * image)):
            parts[0][place0, pl.ds((at + 1) * tiles + tile, 1), :] = jnp.sum(value, axis=0, keepdims=True)

    image_pair = pair_copy(1, images.at[:, own_cols], images.at[:, own_cols])
    image_pair.start()

    for phase, (place, count, device_of) in enumerate(phases):
        copies = []
        for step in range(1, count):
            copies.append(pltpu.make_async_remote_copy(
                src_ref=parts[phase].at[place], dst_ref=parts[phase].at[place],
                send_sem=part_send[phase].at[step], recv_sem=part_recv[phase].at[step],
                device_id=device_of(lax.rem(place + step, count)), device_id_type=MESH,
            ))
        for copy in copies:
            copy.start()
        for copy in copies:
            copy.wait()
        total = parts[phase][0]
        for index in range(1, count):
            total = total + parts[phase][index]
        if phase + 1 < phase_count:
            parts[phase + 1][phases[phase + 1][0]] = total
        else:
            totals[rep] = total

    total_pair = pair_copy(2, totals.at[rep], totals.at[rep])
    total_pair.start()

    load_dir_other.wait()
    load_sol.wait()

    def make_factors(side):
        for tile in range(tiles):
            norm_old, curvature, crossing, image_square = (
                totals[side, pl.ds(at * tiles + tile, 1), :] for at in range(4)
            )
            step_size = norm_old / curvature
            norm_new = norm_old - 2.0 * step_size * crossing + step_size * step_size * image_square
            cols = tile_cols(side, tile)
            steps[:, cols] = step_size
            scales[:, cols] = norm_new / norm_old

    make_factors(rep)
    image_pair.wait()
    total_pair.wait()
    make_factors(other)

    for chunk in range(chunks):
        near_copy(chunk).wait_send()

        @pl.when(sends_far)
        def _():
            far_copy(chunk).wait_send()


def solution(mesh):
    sizes = (mesh.shape["row"], mesh.shape["col"])
    segments = sizes[0] * sizes[1]
    counts = (segments,) if segments <= DIRECT_LIMIT else (sizes[1], sizes[0])

    def per_device(gain, coupled_columns, solution, residual, direction):
        seg_rows, snapshots = direction.shape
        half = snapshots // 2
        block_rows, slots_half = gain.shape[:2]
        chunks = seg_rows // CHUNK_ROWS
        sum_rows = 4 * (half // LANES)
        dma = pltpu.SemaphoreType.DMA
        whole = pltpu.VMEM((seg_rows, snapshots), jnp.float32)
        line = pltpu.VMEM((1, snapshots), jnp.float32)
        any_space = pl.BlockSpec(memory_space=pl.ANY)
        vmem = pl.BlockSpec(memory_space=pltpu.VMEM)
        held, residual_held, solution_held, image, steps, scales = pl.pallas_call(
            functools.partial(iteration_kernel, sizes),
            out_shape=(whole, whole, whole, whole, line, line),
            in_specs=[pl.BlockSpec(memory_space=pltpu.SMEM), any_space, any_space, any_space, any_space],
            out_specs=(vmem,) * 6,
            scratch_shapes=[
                pltpu.VMEM((2, block_rows, slots_half, BLK, BLK), jnp.float32),
                pltpu.VMEM((seg_rows, half), jnp.float32),
                pltpu.VMEM((seg_rows, half), jnp.float32),
                pltpu.VMEM((3, seg_rows, seg_rows), jnp.bfloat16),
                pltpu.VMEM((3, seg_rows, seg_rows), jnp.bfloat16),
                pltpu.VMEM((2, sum_rows, LANES), jnp.float32),
                *[pltpu.VMEM((count, sum_rows, LANES), jnp.float32) for count in counts],
                *[dma((count,)) for count in counts],
                *[dma((count,)) for count in counts],
                dma((chunks,)), dma((chunks,)), dma((chunks,)), dma((chunks,)),
                dma((3,)), dma((3,)), dma((5,)),
            ],
            compiler_params=pltpu.CompilerParams(collective_id=0, has_side_effects=True),
            name="cg_iteration",
        )(coupled_columns, gain, solution, residual, direction)
        residual_next = residual_held - steps * image
        return solution_held + steps * held, residual_next, residual_next + scales * held

    return jax.shard_map(
        per_device,
        mesh=mesh,
        in_specs=(
            P(("row", "col"), "rep", None, None),
            P(("row", "col"), None),
            P(("row", "col"), None),
            P(("row", "col"), None),
            P(("row", "col"), None),
        ),
        out_specs=(P(("row", "col"), None), P(("row", "col"), None), P(("row", "col"), None)),
        check_vma=False,
    )
```

```python
import functools

import jax
import jax.numpy as jnp
from jax import lax
from jax.experimental import pallas as pl
from jax.experimental.pallas import tpu as pltpu
from jax.sharding import PartitionSpec as P

BLK = 128
LANES = 128
DIRECT_LIMIT = 16
CHUNK_ROWS = 32
MESH = pl.DeviceIdType.MESH


def split_bf16(value):
    high = value.astype(jnp.bfloat16)
    low = (value - high.astype(jnp.float32)).astype(jnp.bfloat16)
    return high, low


def iteration_kernel(
    sizes,
    columns_ref, gain_hbm, solution_hbm, residual_hbm, direction_hbm,
    own_dir, own_res, own_sol, images, steps, scales,
    gains, near, far, band_high, band_low, totals, *rest,
):
    rows_n, cols_n = sizes
    segments = rows_n * cols_n
    direct = segments <= DIRECT_LIMIT
    phase_count = 1 if direct else 2
    parts = rest[:phase_count]
    part_send = rest[phase_count:2 * phase_count]
    part_recv = rest[2 * phase_count:3 * phase_count]
    (near_send, near_recv, far_send, far_recv, pair_send, pair_recv, local_sem, known) = rest[3 * phase_count:]

    seg_rows, half = near.shape
    block_rows = seg_rows // BLK
    slots_half = gains.shape[2]
    tiles = half // LANES
    chunks = seg_rows // CHUNK_ROWS

    row, col, rep = lax.axis_index("row"), lax.axis_index("col"), lax.axis_index("rep")
    seg = row * cols_n + col
    odd = lax.rem(seg, 2)
    other = 1 - rep

    def at_segment(index):
        return {"row": index // cols_n, "col": lax.rem(index, cols_n), "rep": rep}

    partner = {"row": row, "col": col, "rep": other}
    near_id = at_segment(seg + 1 - 2 * odd)
    target = seg + 2 - 4 * odd
    source = seg - 2 + 4 * odd
    sends_far = jnp.logical_and(target >= 0, target < segments)
    gets_far = jnp.logical_and(source >= 0, source < segments)
    far_id = at_segment(jnp.clip(target, 0, segments - 1))
    source_id = at_segment(jnp.clip(source, 0, segments - 1))

    if direct:
        phases = [(seg, segments, at_segment)]
    else:
        phases = [
            (col, cols_n, lambda index: {"row": row, "col": index, "rep": rep}),
            (row, rows_n, lambda index: {"row": index, "col": col, "rep": rep}),
        ]

    barrier = pltpu.get_barrier_semaphore()

    def greet(device):
        pl.semaphore_signal(barrier, inc=1, device_id=device, device_id_type=MESH)

    own_cols = pl.ds(pl.multiple_of(rep * half, LANES), half)
    other_cols = pl.ds(pl.multiple_of(other * half, LANES), half)
    load_dir = pltpu.make_async_copy(direction_hbm.at[:, own_cols], own_dir.at[:, own_cols], local_sem.at[0])
    load_gain = pltpu.make_async_copy(gain_hbm, gains.at[rep], local_sem.at[1])
    load_res = pltpu.make_async_copy(residual_hbm, own_res, local_sem.at[2])
    load_dir_other = pltpu.make_async_copy(direction_hbm.at[:, other_cols], own_dir.at[:, other_cols], local_sem.at[3])
    load_sol = pltpu.make_async_copy(solution_hbm, own_sol, local_sem.at[4])

    greet(partner)
    if direct:
        steps_around = [
            (jnp.bool_(True), {"row": row, "col": col + 1 - 2 * odd, "rep": rep}),
            (col >= 2, {"row": row, "col": jnp.maximum(col - 2, 0), "rep": rep}),
            (col + 2 < cols_n, {"row": row, "col": jnp.minimum(col + 2, cols_n - 1), "rep": rep}),
            (row >= 1, {"row": jnp.maximum(row - 1, 0), "col": col, "rep": rep}),
            (row + 1 < rows_n, {"row": jnp.minimum(row + 1, rows_n - 1), "col": col, "rep": rep}),
        ]

        near_count = sum(exists.astype(jnp.int32) for exists, device in steps_around)

        def around(act):
            for exists, device in steps_around:
                @pl.when(exists)
                def _(device=device):
                    act(device)

        around(greet)
    else:
        greet(near_id)
        for place, count, device_of in phases:
            for step in range(1, count):
                greet(device_of(lax.rem(place + step, count)))

        @pl.when(sends_far)
        def _():
            greet(far_id)

        @pl.when(gets_far)
        def _():
            greet(source_id)

    load_dir.start()
    load_gain.start()
    load_res.start()
    load_dir_other.start()
    load_sol.start()

    if direct:
        pl.semaphore_wait(barrier, 1 + near_count)
    else:
        pl.semaphore_wait(barrier, 2 + sum(count - 1 for place, count, device_of in phases))

        @pl.when(sends_far)
        def _():
            pl.semaphore_wait(barrier, 1)

        @pl.when(gets_far)
        def _():
            pl.semaphore_wait(barrier, 1)

    def spread(step):
        around(lambda device: pl.semaphore_signal(
            known.at[step], inc=1, device_id=device, device_id_type=MESH))

    def learn(step):
        pl.semaphore_wait(known.at[step], near_count)

    def near_copy(chunk):
        part = pl.ds(chunk * CHUNK_ROWS, CHUNK_ROWS)
        return pltpu.make_async_remote_copy(
            src_ref=own_dir.at[part, own_cols], dst_ref=near.at[part],
            send_sem=near_send.at[chunk], recv_sem=near_recv.at[chunk],
            device_id=near_id, device_id_type=MESH,
        )

    def far_copy(chunk):
        part = pl.ds(chunk * CHUNK_ROWS, CHUNK_ROWS)
        return pltpu.make_async_remote_copy(
            src_ref=near.at[part], dst_ref=far.at[part],
            send_sem=far_send.at[chunk], recv_sem=far_recv.at[chunk],
            device_id=far_id, device_id_type=MESH,
        )

    def pair_copy(index, src, dst):
        return pltpu.make_async_remote_copy(
            src_ref=src, dst_ref=dst, send_sem=pair_send.at[index], recv_sem=pair_recv.at[index],
            device_id=partner, device_id_type=MESH,
        )

    load_dir.wait()
    for chunk in range(chunks):
        near_copy(chunk).start()
    gain_pair = pair_copy(0, gain_hbm, gains.at[rep])
    gain_pair.start()

    rounds = rows_n + cols_n // 2 - 2 if direct else 0
    for step in range(rounds):
        spread(step)
        if step < rounds - 1:
            learn(step)

    first_block = seg * block_rows
    bases = (first_block, first_block + block_rows * (1 - 2 * odd), first_block - block_rows * (1 - 2 * odd))

    def build_band(group):
        for r in range(block_rows):
            names = [columns_ref[r, k] for k in range(2 * slots_half)]
            for j in range(block_rows):
                wanted = bases[group] + j
                slot = jnp.int32(0)
                found = jnp.float32(0)
                for k in reversed(range(2 * slots_half)):
                    match = names[k] == wanted
                    slot = jnp.where(match, k, slot)
                    found = jnp.where(match, jnp.float32(1), found)
                block = gains[slot // slots_half, r, lax.rem(slot, slots_half)] * found
                high, low = split_bf16(block)
                at = (group, pl.ds(r * BLK, BLK), pl.ds(j * BLK, BLK))
                band_high[at] = high
                band_low[at] = low

    def product(group, value):
        high, low = split_bf16(value)
        dot = functools.partial(jnp.dot, preferred_element_type=jnp.float32)
        return dot(band_high[group], high) + (dot(band_high[group], low) + dot(band_low[group], high))

    def tile_cols(side, tile):
        return pl.ds(pl.multiple_of(side * half + tile * LANES, LANES), LANES)

    def start_parts():
        load_res.wait()
        for tile in range(tiles):
            value = own_res[:, tile_cols(rep, tile)]
            parts[0][phases[0][0], pl.ds(tile, 1), :] = jnp.sum(value * value, axis=0, keepdims=True)

    def own_product():
        images[:, own_cols] = product(0, own_dir[:, own_cols])

    def gain_ready():
        load_gain.wait()
        gain_pair.wait()
        build_band(0)

    pieces = {0: start_parts, 1: gain_ready, 2: own_product, 3: lambda: build_band(1), 4: lambda: build_band(2)}
    for chunk in range(chunks):
        near_copy(chunk).wait_recv()

        @pl.when(sends_far)
        def _():
            far_copy(chunk).start()

        if chunk in pieces:
            pieces[chunk]()
    images[:, own_cols] += product(1, near[...])

    @pl.when(gets_far)
    def _():
        for chunk in range(chunks):
            far_copy(chunk).wait_recv()

    @pl.when(jnp.logical_not(gets_far))
    def _():
        far[...] = jnp.zeros_like(far)

    images[:, own_cols] += product(2, far[...])

    if rounds:
        learn(rounds - 1)
    place0 = phases[0][0]
    for tile in range(tiles):
        cols = tile_cols(rep, tile)
        image = images[:, cols]
        for at, value in enumerate((own_dir[:, cols] * image, own_res[:, cols] * image, image * image)):
            parts[0][place0, pl.ds((at + 1) * tiles + tile, 1), :] = jnp.sum(value, axis=0, keepdims=True)

    image_pair = pair_copy(1, images.at[:, own_cols], images.at[:, own_cols])
    image_pair.start()

    for phase, (place, count, device_of) in enumerate(phases):
        copies = []
        for step in range(1, count):
            copies.append(pltpu.make_async_remote_copy(
                src_ref=parts[phase].at[place], dst_ref=parts[phase].at[place],
                send_sem=part_send[phase].at[step], recv_sem=part_recv[phase].at[step],
                device_id=device_of(lax.rem(place + step, count)), device_id_type=MESH,
            ))
        for copy in copies:
            copy.start()
        for copy in copies:
            copy.wait()
        total = parts[phase][0]
        for index in range(1, count):
            total = total + parts[phase][index]
        if phase + 1 < phase_count:
            parts[phase + 1][phases[phase + 1][0]] = total
        else:
            totals[rep] = total

    total_pair = pair_copy(2, totals.at[rep], totals.at[rep])
    total_pair.start()

    load_dir_other.wait()
    load_sol.wait()

    def make_factors(side):
        for tile in range(tiles):
            norm_old, curvature, crossing, image_square = (
                totals[side, pl.ds(at * tiles + tile, 1), :] for at in range(4)
            )
            step_size = norm_old / curvature
            norm_new = norm_old - 2.0 * step_size * crossing + step_size * step_size * image_square
            cols = tile_cols(side, tile)
            steps[:, cols] = step_size
            scales[:, cols] = norm_new / norm_old

    make_factors(rep)
    image_pair.wait()
    total_pair.wait()
    make_factors(other)

    for chunk in range(chunks):
        near_copy(chunk).wait_send()

        @pl.when(sends_far)
        def _():
            far_copy(chunk).wait_send()


def solution(mesh):
    sizes = (mesh.shape["row"], mesh.shape["col"])
    segments = sizes[0] * sizes[1]
    rounds = max(sizes[0] + sizes[1] // 2 - 2, 1)
    counts = (segments,) if segments <= DIRECT_LIMIT else (sizes[1], sizes[0])

    def per_device(gain, coupled_columns, solution, residual, direction):
        seg_rows, snapshots = direction.shape
        half = snapshots // 2
        block_rows, slots_half = gain.shape[:2]
        chunks = seg_rows // CHUNK_ROWS
        sum_rows = 4 * (half // LANES)
        dma = pltpu.SemaphoreType.DMA
        whole = pltpu.VMEM((seg_rows, snapshots), jnp.float32)
        line = pltpu.VMEM((1, snapshots), jnp.float32)
        any_space = pl.BlockSpec(memory_space=pl.ANY)
        vmem = pl.BlockSpec(memory_space=pltpu.VMEM)
        held, residual_held, solution_held, image, steps, scales = pl.pallas_call(
            functools.partial(iteration_kernel, sizes),
            out_shape=(whole, whole, whole, whole, line, line),
            in_specs=[pl.BlockSpec(memory_space=pltpu.SMEM), any_space, any_space, any_space, any_space],
            out_specs=(vmem,) * 6,
            scratch_shapes=[
                pltpu.VMEM((2, block_rows, slots_half, BLK, BLK), jnp.float32),
                pltpu.VMEM((seg_rows, half), jnp.float32),
                pltpu.VMEM((seg_rows, half), jnp.float32),
                pltpu.VMEM((3, seg_rows, seg_rows), jnp.bfloat16),
                pltpu.VMEM((3, seg_rows, seg_rows), jnp.bfloat16),
                pltpu.VMEM((2, sum_rows, LANES), jnp.float32),
                *[pltpu.VMEM((count, sum_rows, LANES), jnp.float32) for count in counts],
                *[dma((count,)) for count in counts],
                *[dma((count,)) for count in counts],
                dma((chunks,)), dma((chunks,)), dma((chunks,)), dma((chunks,)),
                dma((3,)), dma((3,)), dma((5,)), pltpu.SemaphoreType.REGULAR((rounds,)),
            ],
            compiler_params=pltpu.CompilerParams(collective_id=0, has_side_effects=True),
            name="cg_iteration",
        )(coupled_columns, gain, solution, residual, direction)
        residual_next = residual_held - steps * image
        return solution_held + steps * held, residual_next, residual_next + scales * held

    return jax.shard_map(
        per_device,
        mesh=mesh,
        in_specs=(
            P(("row", "col"), "rep", None, None),
            P(("row", "col"), None),
            P(("row", "col"), None),
            P(("row", "col"), None),
            P(("row", "col"), None),
        ),
        out_specs=(P(("row", "col"), None), P(("row", "col"), None), P(("row", "col"), None)),
        check_vma=False,
    )
```

```python
import functools

import jax
import jax.numpy as jnp
from jax import lax
from jax.experimental import pallas as pl
from jax.experimental.pallas import tpu as pltpu
from jax.sharding import PartitionSpec as P

BLK = 128
LANES = 128
DIRECT_LIMIT = 16
CHUNK_ROWS = 64
MESH = pl.DeviceIdType.MESH


def split_bf16(value):
    high = value.astype(jnp.bfloat16)
    low = (value - high.astype(jnp.float32)).astype(jnp.bfloat16)
    return high, low


def iteration_kernel(
    sizes,
    columns_ref, gain_hbm, solution_hbm, residual_hbm, direction_hbm,
    own_dir, own_res, own_sol, images, steps, scales,
    gains, near, far, band_high, band_low, totals, *rest,
):
    rows_n, cols_n = sizes
    segments = rows_n * cols_n
    direct = segments <= DIRECT_LIMIT
    phase_count = 1 if direct else 2
    parts = rest[:phase_count]
    part_send = rest[phase_count:2 * phase_count]
    part_recv = rest[2 * phase_count:3 * phase_count]
    (near_send, near_recv, far_send, far_recv, pair_send, pair_recv, local_sem, known) = rest[3 * phase_count:]

    seg_rows, half = near.shape
    block_rows = seg_rows // BLK
    slots_half = gains.shape[2]
    tiles = half // LANES
    chunks = seg_rows // CHUNK_ROWS

    row, col, rep = lax.axis_index("row"), lax.axis_index("col"), lax.axis_index("rep")
    seg = row * cols_n + col
    odd = lax.rem(seg, 2)
    other = 1 - rep

    def at_segment(index):
        return {"row": index // cols_n, "col": lax.rem(index, cols_n), "rep": rep}

    partner = {"row": row, "col": col, "rep": other}
    near_id = at_segment(seg + 1 - 2 * odd)
    target = seg + 2 - 4 * odd
    source = seg - 2 + 4 * odd
    sends_far = jnp.logical_and(target >= 0, target < segments)
    gets_far = jnp.logical_and(source >= 0, source < segments)
    far_id = at_segment(jnp.clip(target, 0, segments - 1))
    source_id = at_segment(jnp.clip(source, 0, segments - 1))

    if direct:
        phases = [(seg, segments, at_segment)]
    else:
        phases = [
            (col, cols_n, lambda index: {"row": row, "col": index, "rep": rep}),
            (row, rows_n, lambda index: {"row": index, "col": col, "rep": rep}),
        ]

    barrier = pltpu.get_barrier_semaphore()

    def greet(device):
        pl.semaphore_signal(barrier, inc=1, device_id=device, device_id_type=MESH)

    own_cols = pl.ds(pl.multiple_of(rep * half, LANES), half)
    other_cols = pl.ds(pl.multiple_of(other * half, LANES), half)
    load_dir = pltpu.make_async_copy(direction_hbm.at[:, own_cols], own_dir.at[:, own_cols], local_sem.at[0])
    load_gain = pltpu.make_async_copy(gain_hbm, gains.at[rep], local_sem.at[1])
    load_res = pltpu.make_async_copy(residual_hbm, own_res, local_sem.at[2])
    load_dir_other = pltpu.make_async_copy(direction_hbm.at[:, other_cols], own_dir.at[:, other_cols], local_sem.at[3])
    load_sol = pltpu.make_async_copy(solution_hbm, own_sol, local_sem.at[4])

    greet(partner)
    if direct:
        steps_around = [
            (jnp.bool_(True), {"row": row, "col": col + 1 - 2 * odd, "rep": rep}),
            (col >= 2, {"row": row, "col": jnp.maximum(col - 2, 0), "rep": rep}),
            (col + 2 < cols_n, {"row": row, "col": jnp.minimum(col + 2, cols_n - 1), "rep": rep}),
            (row >= 1, {"row": jnp.maximum(row - 1, 0), "col": col, "rep": rep}),
            (row + 1 < rows_n, {"row": jnp.minimum(row + 1, rows_n - 1), "col": col, "rep": rep}),
        ]

        near_count = sum(exists.astype(jnp.int32) for exists, device in steps_around)

        def around(act):
            for exists, device in steps_around:
                @pl.when(exists)
                def _(device=device):
                    act(device)

        around(greet)
    else:
        greet(near_id)
        for place, count, device_of in phases:
            for step in range(1, count):
                greet(device_of(lax.rem(place + step, count)))

        @pl.when(sends_far)
        def _():
            greet(far_id)

        @pl.when(gets_far)
        def _():
            greet(source_id)

    load_dir.start()
    load_gain.start()
    load_res.start()
    load_dir_other.start()
    load_sol.start()

    if direct:
        pl.semaphore_wait(barrier, 1 + near_count)
    else:
        pl.semaphore_wait(barrier, 2 + sum(count - 1 for place, count, device_of in phases))

        @pl.when(sends_far)
        def _():
            pl.semaphore_wait(barrier, 1)

        @pl.when(gets_far)
        def _():
            pl.semaphore_wait(barrier, 1)

    def spread(step):
        around(lambda device: pl.semaphore_signal(
            known.at[step], inc=1, device_id=device, device_id_type=MESH))

    def learn(step):
        pl.semaphore_wait(known.at[step], near_count)

    def near_copy(chunk):
        part = pl.ds(chunk * CHUNK_ROWS, CHUNK_ROWS)
        return pltpu.make_async_remote_copy(
            src_ref=own_dir.at[part, own_cols], dst_ref=near.at[part],
            send_sem=near_send.at[chunk], recv_sem=near_recv.at[chunk],
            device_id=near_id, device_id_type=MESH,
        )

    def far_copy(chunk):
        part = pl.ds(chunk * CHUNK_ROWS, CHUNK_ROWS)
        return pltpu.make_async_remote_copy(
            src_ref=near.at[part], dst_ref=far.at[part],
            send_sem=far_send.at[chunk], recv_sem=far_recv.at[chunk],
            device_id=far_id, device_id_type=MESH,
        )

    def pair_copy(index, src, dst):
        return pltpu.make_async_remote_copy(
            src_ref=src, dst_ref=dst, send_sem=pair_send.at[index], recv_sem=pair_recv.at[index],
            device_id=partner, device_id_type=MESH,
        )

    load_dir.wait()
    for chunk in range(chunks):
        near_copy(chunk).start()
    gain_pair = pair_copy(0, gain_hbm, gains.at[rep])
    gain_pair.start()

    rounds = rows_n + cols_n // 2 - 2 if direct else 0
    for step in range(rounds):
        spread(step)
        if step < rounds - 1:
            learn(step)

    first_block = seg * block_rows
    bases = (first_block, first_block + block_rows * (1 - 2 * odd), first_block - block_rows * (1 - 2 * odd))

    def build_band(group):
        for r in range(block_rows):
            names = [columns_ref[r, k] for k in range(2 * slots_half)]
            for j in range(block_rows):
                wanted = bases[group] + j
                slot = jnp.int32(0)
                found = jnp.float32(0)
                for k in reversed(range(2 * slots_half)):
                    match = names[k] == wanted
                    slot = jnp.where(match, k, slot)
                    found = jnp.where(match, jnp.float32(1), found)
                block = gains[slot // slots_half, r, lax.rem(slot, slots_half)] * found
                high, low = split_bf16(block)
                at = (group, pl.ds(r * BLK, BLK), pl.ds(j * BLK, BLK))
                band_high[at] = high
                band_low[at] = low

    def product(group, value):
        high, low = split_bf16(value)
        dot = functools.partial(jnp.dot, preferred_element_type=jnp.float32)
        return dot(band_high[group], high) + (dot(band_high[group], low) + dot(band_low[group], high))

    def tile_cols(side, tile):
        return pl.ds(pl.multiple_of(side * half + tile * LANES, LANES), LANES)

    def start_parts():
        load_res.wait()
        for tile in range(tiles):
            value = own_res[:, tile_cols(rep, tile)]
            parts[0][phases[0][0], pl.ds(tile, 1), :] = jnp.sum(value * value, axis=0, keepdims=True)

    def own_product():
        images[:, own_cols] = product(0, own_dir[:, own_cols])

    def gain_ready():
        load_gain.wait()
        gain_pair.wait()
        build_band(0)

    pieces = {0: start_parts, 1: gain_ready, 2: own_product, 3: lambda: build_band(1), 4: lambda: build_band(2)}
    for chunk in range(chunks):
        near_copy(chunk).wait_recv()

        @pl.when(sends_far)
        def _():
            far_copy(chunk).start()

        if chunk in pieces:
            pieces[chunk]()
    images[:, own_cols] += product(1, near[...])

    @pl.when(gets_far)
    def _():
        for chunk in range(chunks):
            far_copy(chunk).wait_recv()

    @pl.when(jnp.logical_not(gets_far))
    def _():
        far[...] = jnp.zeros_like(far)

    images[:, own_cols] += product(2, far[...])

    if rounds:
        learn(rounds - 1)
    place0 = phases[0][0]
    for tile in range(tiles):
        cols = tile_cols(rep, tile)
        image = images[:, cols]
        for at, value in enumerate((own_dir[:, cols] * image, own_res[:, cols] * image, image * image)):
            parts[0][place0, pl.ds((at + 1) * tiles + tile, 1), :] = jnp.sum(value, axis=0, keepdims=True)

    image_pair = pair_copy(1, images.at[:, own_cols], images.at[:, own_cols])
    image_pair.start()

    for phase, (place, count, device_of) in enumerate(phases):
        copies = []
        for step in range(1, count):
            copies.append(pltpu.make_async_remote_copy(
                src_ref=parts[phase].at[place], dst_ref=parts[phase].at[place],
                send_sem=part_send[phase].at[step], recv_sem=part_recv[phase].at[step],
                device_id=device_of(lax.rem(place + step, count)), device_id_type=MESH,
            ))
        for copy in reversed(copies):
            copy.start()
        for copy in copies:
            copy.wait()
        total = parts[phase][0]
        for index in range(1, count):
            total = total + parts[phase][index]
        if phase + 1 < phase_count:
            parts[phase + 1][phases[phase + 1][0]] = total
        else:
            totals[rep] = total

    total_pair = pair_copy(2, totals.at[rep], totals.at[rep])
    total_pair.start()

    load_dir_other.wait()
    load_sol.wait()

    def make_factors(side):
        for tile in range(tiles):
            norm_old, curvature, crossing, image_square = (
                totals[side, pl.ds(at * tiles + tile, 1), :] for at in range(4)
            )
            step_size = norm_old / curvature
            norm_new = norm_old - 2.0 * step_size * crossing + step_size * step_size * image_square
            cols = tile_cols(side, tile)
            steps[:, cols] = step_size
            scales[:, cols] = norm_new / norm_old

    make_factors(rep)
    image_pair.wait()
    total_pair.wait()
    make_factors(other)

    for chunk in range(chunks):
        near_copy(chunk).wait_send()

        @pl.when(sends_far)
        def _():
            far_copy(chunk).wait_send()


def solution(mesh):
    sizes = (mesh.shape["row"], mesh.shape["col"])
    segments = sizes[0] * sizes[1]
    rounds = max(sizes[0] + sizes[1] // 2 - 2, 1)
    counts = (segments,) if segments <= DIRECT_LIMIT else (sizes[1], sizes[0])

    def per_device(gain, coupled_columns, solution, residual, direction):
        seg_rows, snapshots = direction.shape
        half = snapshots // 2
        block_rows, slots_half = gain.shape[:2]
        chunks = seg_rows // CHUNK_ROWS
        sum_rows = 4 * (half // LANES)
        dma = pltpu.SemaphoreType.DMA
        whole = pltpu.VMEM((seg_rows, snapshots), jnp.float32)
        line = pltpu.VMEM((1, snapshots), jnp.float32)
        any_space = pl.BlockSpec(memory_space=pl.ANY)
        vmem = pl.BlockSpec(memory_space=pltpu.VMEM)
        held, residual_held, solution_held, image, steps, scales = pl.pallas_call(
            functools.partial(iteration_kernel, sizes),
            out_shape=(whole, whole, whole, whole, line, line),
            in_specs=[pl.BlockSpec(memory_space=pltpu.SMEM), any_space, any_space, any_space, any_space],
            out_specs=(vmem,) * 6,
            scratch_shapes=[
                pltpu.VMEM((2, block_rows, slots_half, BLK, BLK), jnp.float32),
                pltpu.VMEM((seg_rows, half), jnp.float32),
                pltpu.VMEM((seg_rows, half), jnp.float32),
                pltpu.VMEM((3, seg_rows, seg_rows), jnp.bfloat16),
                pltpu.VMEM((3, seg_rows, seg_rows), jnp.bfloat16),
                pltpu.VMEM((2, sum_rows, LANES), jnp.float32),
                *[pltpu.VMEM((count, sum_rows, LANES), jnp.float32) for count in counts],
                *[dma((count,)) for count in counts],
                *[dma((count,)) for count in counts],
                dma((chunks,)), dma((chunks,)), dma((chunks,)), dma((chunks,)),
                dma((3,)), dma((3,)), dma((5,)), pltpu.SemaphoreType.REGULAR((rounds,)),
            ],
            compiler_params=pltpu.CompilerParams(collective_id=0, has_side_effects=True),
            name="cg_iteration",
        )(coupled_columns, gain, solution, residual, direction)
        residual_next = residual_held - steps * image
        return solution_held + steps * held, residual_next, residual_next + scales * held

    return jax.shard_map(
        per_device,
        mesh=mesh,
        in_specs=(
            P(("row", "col"), "rep", None, None),
            P(("row", "col"), None),
            P(("row", "col"), None),
            P(("row", "col"), None),
            P(("row", "col"), None),
        ),
        out_specs=(P(("row", "col"), None), P(("row", "col"), None), P(("row", "col"), None)),
        check_vma=False,
    )
```
